32 devices in a mesh: grp: 4 (over z), wave: 8 (over y, x, core).
Axes of the slice: x: 2, y: 2, z: 4, core: 2. Of those that a mesh axis runs over, the one named last changes fastest.
Arguments:
- state: bfloat16 [275, 61760], P(None, ('grp', 'wave')), may hold values from -6 to 6
- held_orders: int32 [160], P(('grp', 'wave')), may hold values from -1 to 95, as said below
- pair_lows: int32 [96], P(('grp', 'wave')), may hold values from 0 to 95, each once
- inverses: bfloat16 [96, 2, 137, 137], P(('grp', 'wave')), may hold values from -2 to 3
- height_operator: bfloat16 [137, 137], replicated, may hold values from -0.5 to 0.5
- pressure_column: bfloat16 [137], replicated, may hold values from -5 to 5
- thermal_response_matrix: bfloat16 [137, 137], replicated, may hold values from -0.5 to 0.5
- mass_row: bfloat16 [137], replicated, may hold values from -0.5 to 0.5
Outputs:
- advanced: bfloat16 [275, 61760], P(None, ('grp', 'wave'))
The draws below stay inside these ranges and needn't reach their ends.
Inputs may be any that keep to these rules, and one draw needn't show every extreme that they name: `held_orders`: each of 0 to 95 appears exactly once, all other entries are -1; some device has all 5 of its slots filled.
All inputs are finite; a program needn't handle non-finite values.
Results may differ from the reference program's by a relative error of at most 0.0052.
Values may be sent and summed in bfloat16 or wider, within the bound.
A program may use at most 128 MiB of HBM per device.

```python
import jax
import jax.numpy as jnp
from jax import lax

LEVELS = 137
KMAX = 5
HALF = 96
TRUNC = 191
ORDER_SLOTS = 160
WIDTH_SLOT = 386
COLS = 61760


def draw_held_orders(key, part):
    key_a, key_b, key_c = jax.random.split(jax.random.fold_in(key, 11), 3)
    slot_total = ORDER_SLOTS
    device_total = slot_total // KMAX
    scores = jax.random.permutation(key_a, slot_total).astype(jnp.int32)
    full_device = jax.random.randint(key_b, (), 0, device_total)
    owners = jnp.arange(slot_total, dtype=jnp.int32) // KMAX
    scores = scores - jnp.where(owners == full_device, slot_total, 0).astype(jnp.int32)
    ranking = jnp.argsort(jnp.argsort(scores))
    filled = ranking < HALF
    serial = jnp.cumsum(filled.astype(jnp.int32)) - 1
    orders = jax.random.permutation(key_c, HALF).astype(jnp.int32)
    picked = orders[jnp.clip(serial, 0, HALF - 1)]
    return jnp.where(filled, picked, -1).astype(jnp.int32)


def draw_inverses(key, part):
    key_a, key_b = jax.random.split(jax.random.fold_in(key, 23))
    diagonal = jax.random.uniform(key_a, (HALF, 2, LEVELS), jnp.float32, 0.6, 1.4)
    spread = jnp.clip(jax.random.normal(key_b, (HALF, 2, LEVELS, LEVELS), jnp.float32), -6.0, 6.0) * (0.6 / LEVELS ** 0.5)
    identity = jnp.eye(LEVELS, dtype=jnp.float32)
    return (spread + diagonal[..., None] * identity).astype(jnp.bfloat16)


def levels(rng, dims, pieces, low, top_value):
    level = 1.0
    for dim, parts in pieces:
        draws = jax.random.uniform(jax.random.fold_in(jax.random.fold_in(rng, 6), dim), (parts,), jnp.float32, low / len(pieces), top_value / len(pieces))
        level = level * jnp.repeat(jnp.exp(draws), dims[dim] // parts).reshape((-1,) + (1,) * (len(dims) - 1 - dim))
    return level


def noise(own_key, dims, deviation, most, pieces=(), held_as=jnp.bfloat16):
    loudness = levels(own_key, dims, pieces, -0.22, 0.18) if pieces else 1.0
    drawn = jax.random.normal(own_key, dims, jnp.float32) * deviation * loudness
    return jnp.minimum(jnp.maximum(drawn, -most), most).astype(held_as)


def setup_inputs(seed: int = 0) -> dict:
    splits = jax.random.split(jax.random.key(seed), 9)
    state = noise(splits[0], (2 * LEVELS + 1, COLS), 1.0, 6.0, ((1, 32),))
    held_orders = draw_held_orders(jax.random.fold_in(splits[8], 71), 0)
    pair_lows = jax.random.permutation(splits[2], HALF).astype(jnp.int32)
    inverses = draw_inverses(jax.random.fold_in(splits[8], 71), 0)
    height_operator = noise(splits[4], (LEVELS, LEVELS), LEVELS ** -0.5, 0.5)
    pressure_column = noise(splits[5], (LEVELS,), 1.0, 5.0)
    thermal_response_matrix = noise(splits[6], (LEVELS, LEVELS), LEVELS ** -0.5, 0.5)
    mass_row = noise(splits[7], (LEVELS,), LEVELS ** -0.5, 0.5)
    return {"state": state, "held_orders": held_orders, "pair_lows": pair_lows, "inverses": inverses, "height_operator": height_operator, "pressure_column": pressure_column, "thermal_response_matrix": thermal_response_matrix, "mass_row": mass_row}


def reference(state, held_orders, pair_lows, inverses, height_operator, pressure_column, thermal_response_matrix, mass_row):
    layer_heights_count = LEVELS
    truncation = TRUNC
    slot_width = WIDTH_SLOT
    slot_of = jnp.zeros((HALF,), jnp.int32).at[jnp.where(held_orders >= 0, held_orders, HALF)].set(
        jnp.arange(ORDER_SLOTS, dtype=jnp.int32), mode="drop")
    pair_of = jnp.zeros((HALF,), jnp.int32).at[pair_lows].set(jnp.arange(HALF, dtype=jnp.int32))
    coeff_index = jnp.arange(slot_width // 2, dtype=jnp.int32)
    denom = float(truncation * (truncation + 1))

    def pair_block(low_degree):
        high_degree = truncation - low_degree
        in_low = coeff_index <= low_degree
        degree = jnp.where(in_low, low_degree, high_degree)
        order_of = jnp.where(in_low, coeff_index, coeff_index - low_degree - 1)
        pair_m = jnp.minimum(order_of, truncation - order_of)
        position = jnp.where(order_of == pair_m, degree - order_of, degree + 1)
        first_col = slot_of[pair_m] * slot_width + 2 * position
        spectral_stacks = jnp.stack([first_col, first_col + 1], axis=1).reshape(-1).astype(jnp.int32)
        grouped_arrays = jnp.take(state, spectral_stacks, axis=1)
        divergence = grouped_arrays[:layer_heights_count]
        thermal_state_array = grouped_arrays[layer_heights_count:2 * layer_heights_count]
        pressure = grouped_arrays[2 * layer_heights_count]
        lap_scale = jnp.repeat((degree * (degree + 1)).astype(jnp.float32) / denom, 2)
        height_drive_term = jnp.dot(height_operator, thermal_state_array, preferred_element_type=jnp.float32)
        height_drive_term = height_drive_term + pressure_column.astype(jnp.float32)[:, None] * pressure.astype(jnp.float32)[None, :]
        right_side = (divergence.astype(jnp.float32) + lap_scale[None, :] * height_drive_term).astype(jnp.bfloat16)
        slot_pair = pair_of[low_degree]
        div_low = jnp.dot(inverses[slot_pair, 0], right_side, preferred_element_type=jnp.float32)
        div_high = jnp.dot(inverses[slot_pair, 1], right_side, preferred_element_type=jnp.float32)
        next_spreading_rate = jnp.where(jnp.repeat(in_low, 2)[None, :], div_low, div_high).astype(jnp.bfloat16)
        next_thermal_state = (thermal_state_array.astype(jnp.float32)
                    - jnp.dot(thermal_response_matrix, next_spreading_rate, preferred_element_type=jnp.float32)).astype(jnp.bfloat16)
        surface_mass_next = (pressure.astype(jnp.float32)
                     - jnp.dot(mass_row, next_spreading_rate, preferred_element_type=jnp.float32)).astype(jnp.bfloat16)
        return jnp.concatenate([next_spreading_rate, next_thermal_state, surface_mass_next[None, :]], axis=0), spectral_stacks

    blocks, spectral_stacks = lax.map(pair_block, jnp.arange(HALF, dtype=jnp.int32))
    rows = 2 * layer_heights_count + 1
    flat = jnp.transpose(blocks, (1, 0, 2)).reshape(rows, -1)
    result = jnp.zeros((rows, COLS), jnp.bfloat16)
    return result.at[:, spectral_stacks.reshape(-1)].set(flat)
```

```python
import functools

import jax
import jax.numpy as jnp
from jax import lax
from jax.experimental import pallas as pl
from jax.experimental.pallas import tpu as pltpu
from jax.sharding import PartitionSpec as P

MESH = pl.DeviceIdType.MESH
LANES = 128
ROWS_TILE = 16
KEEP_BYTES = 24 << 20


def ceil_to(value, step):
    return -(-value // step) * step


def kernel(
    size,
    held,
    lows,
    state,
    inverses,
    height,
    response,
    out,
    info,
    matrices,
    rest,
    right,
    pick,
    outgoing,
    arrived,
    solved,
    returned,
    total,
    info_send,
    info_recv,
    z_send,
    z_recv,
    out_send,
    out_recv,
    back_send,
    back_recv,
):
    Z, W, levels, slots, pairs = size
    half_count = Z * W * pairs
    truncation = 2 * half_count - 1
    slot_width = 2 * (truncation + 2)
    width = slots * slot_width
    denom = float(truncation * (truncation + 1))
    devices = Z * W
    per_pair = 4 * slots
    block_pairs = Z * pairs // 2
    first_extra = block_pairs * per_pair
    tail = levels - LANES
    chunks = pairs + 1
    keep = pick.shape[0] > 1
    z = lax.axis_index("grp")
    w = lax.axis_index("wave")
    me = z * W + w

    barrier = pltpu.get_barrier_semaphore()

    def greet(k, carry):
        other = lax.rem(me + k, devices)
        pl.semaphore_signal(
            barrier, inc=1, device_id=(other // W, lax.rem(other, W)), device_id_type=MESH
        )
        return carry

    lax.fori_loop(1, devices, greet, 0)

    lane = lax.broadcasted_iota(jnp.int32, (1, LANES), 1)
    extra = lane >= first_extra
    used = lane < first_extra + slots
    lane_pair = lane // per_pair
    lane_member = lax.rem(lane, per_pair) // (2 * slots)
    lane_slot = jnp.where(extra, lane - first_extra, lax.rem(lane, 2 * slots) // 2)
    orders = jnp.full((1, LANES), -1, jnp.int32)
    for s in range(slots):
        orders = jnp.where(lane_slot == s, held[s], orders)
    row = lax.broadcasted_iota(jnp.int32, (pairs + 1, LANES), 0)
    tile = jnp.broadcast_to(orders, (pairs + 1, LANES))
    for j in range(pairs):
        tile = jnp.where(row == j, lows[j], tile)
    info[me] = tile

    ends = []
    for i in range(2 * pairs):
        matrices[z, i, 0:levels, :] = inverses[i]
        ends.append(inverses[i, :, LANES:levels].astype(jnp.float32))
    ends = jnp.concatenate(ends, axis=1).astype(jnp.bfloat16)
    rest[z, 0:levels, 0 : 2 * pairs * tail] = ends

    pl.semaphore_wait(barrier, devices - 1)

    def info_copy(k):
        other = lax.rem(me + k, devices)
        return pltpu.make_async_remote_copy(
            src_ref=info.at[me],
            dst_ref=info.at[me],
            send_sem=info_send.at[k],
            recv_sem=info_recv.at[k],
            device_id=(other // W, lax.rem(other, W)),
            device_id_type=MESH,
        )

    def info_arrival(k):
        source = lax.rem(me + devices - k, devices)
        return pltpu.make_async_remote_copy(
            src_ref=info.at[source],
            dst_ref=info.at[source],
            send_sem=info_send.at[k],
            recv_sem=info_recv.at[k],
            device_id=(source // W, lax.rem(source, W)),
            device_id_type=MESH,
        )

    def start_info(k, carry):
        info_copy(k).start()
        return carry

    lax.fori_loop(1, devices, start_info, 0)

    def z_copy(g, c, way):
        if c < pairs:
            ref = matrices.at[g, pl.ds(2 * c, 2), :, pl.ds(0, LANES)]
        else:
            ref = rest.at[g]
        step = 1 if way == 0 else -1
        return pltpu.make_async_remote_copy(
            src_ref=ref,
            dst_ref=ref,
            send_sem=z_send.at[g, c, way],
            recv_sem=z_recv.at[g, c],
            device_id=(z + step, w),
            device_id_type=MESH,
        )

    def forward(g, c):
        @pl.when(jnp.logical_and(g <= z, z < Z - 1))
        def _():
            z_copy(g, c, 0).start()

        @pl.when(jnp.logical_and(g >= z, z > 0))
        def _():
            z_copy(g, c, 1).start()

    def group_at(t):
        g = z
        for zz in range(Z):
            by_distance = sorted(range(Z), key=lambda a: abs(a - zz))
            g = jnp.where(z == zz, by_distance[t], g)
        return g

    def relay(t):
        g = group_at(t)
        for c in range(chunks):
            z_copy(g, c, 0).wait_recv()
            forward(g, c)

    for c in range(chunks):
        forward(z, c)

    column = lax.broadcasted_iota(jnp.int32, (1, width), 1)
    column_order = jnp.full((1, width), -1, jnp.int32)
    column_start = jnp.zeros((1, width), jnp.int32)
    for s in range(slots):
        inside = jnp.logical_and(column >= s * slot_width, column < (s + 1) * slot_width)
        column_order = jnp.where(inside, held[s], column_order)
        column_start = jnp.where(inside, s * slot_width, column_start)
    coefficient = (column - column_start) // 2
    degree = jnp.where(
        coefficient <= truncation - column_order, column_order + coefficient, coefficient - 1
    )
    lap_scale = (degree * (degree + 1)).astype(jnp.float32) / denom
    drive = jnp.dot(height[...], state[LANES:, :], preferred_element_type=jnp.float32)
    right[0:levels, :] = (
        state[0:levels, :].astype(jnp.float32) + lap_scale * drive
    ).astype(jnp.bfloat16)

    def wait_info(k, carry):
        info_arrival(k).wait_recv()
        return carry

    lax.fori_loop(1, devices, wait_info, 0)

    def build(k, place):
        d = lax.rem(w + k, W)
        tables = [info[g * W + d] for g in range(Z)]
        low_rows = [tables[g][j : j + 1] for g in range(Z) for j in range(pairs)]
        hit = low_rows[0] == orders
        for low in low_rows[1:]:
            hit = jnp.logical_or(hit, low == orders)
        for b in range(2):
            low = jnp.zeros((1, LANES), jnp.int32)
            for p in range(block_pairs):
                low = jnp.where(lane_pair == p, low_rows[b * block_pairs + p], low)
            merged = jnp.where(orders <= low, low - orders, truncation + 1 - low)
            position = jnp.where(lane_member == 0, merged, truncation - low - orders)
            position = jnp.where(extra, truncation + 1 - orders, position)
            part = jnp.where(extra, b, lax.rem(lane, 2))
            target = lane_slot * slot_width + 2 * position + part
            target = jnp.where(jnp.logical_and(orders >= 0, used), target, -1)
            target = jnp.where(jnp.logical_and(extra, jnp.logical_not(hit)), -1, target)
            at = lax.broadcasted_iota(jnp.int32, (width, LANES), 0)
            pick[place, :, b * LANES : (b + 1) * LANES] = jnp.where(
                at == target, 1.0, 0.0
            ).astype(jnp.bfloat16)

    def place_of(k):
        return k if keep else 0

    def out_copy(k):
        return pltpu.make_async_remote_copy(
            src_ref=outgoing.at[k],
            dst_ref=arrived.at[k],
            send_sem=out_send.at[k],
            recv_sem=out_recv.at[k],
            device_id=(z, lax.rem(w + k, W)),
            device_id_type=MESH,
        )

    def back_copy(k):
        return pltpu.make_async_remote_copy(
            src_ref=solved.at[k],
            dst_ref=returned.at[k],
            send_sem=back_send.at[k],
            recv_sem=back_recv.at[k],
            device_id=(z, lax.rem(w + W - k, W)),
            device_id_type=MESH,
        )

    def message(k):
        build(k, place_of(k))
        return jnp.dot(
            right[...], pick[place_of(k)], preferred_element_type=jnp.float32
        ).astype(jnp.bfloat16)

    def send(k, carry):
        outgoing[k] = message(k)
        out_copy(k).start()
        return carry

    middle = W // 2 + 1
    lax.fori_loop(1, middle, send, 0)
    relay(1)
    lax.fori_loop(middle, W, send, 0)
    arrived[0] = message(0)

    for t in range(2, Z - 1):
        relay(t)

    def wait_out(k, carry):
        out_copy(k).wait_recv()
        return carry

    lax.fori_loop(1, W, wait_out, 0)

    wide_lane = jnp.concatenate([lane, lane], axis=1)
    wide_pair = wide_lane // per_pair
    wide_member = lax.rem(wide_lane, per_pair) // (2 * slots)
    wide_extra = jnp.logical_and(wide_lane >= first_extra, wide_lane < first_extra + slots)

    def solve(t):
        g = group_at(t)
        b = (g * pairs) // block_pairs
        for i in range(2 * pairs):
            if t > 0:
                piece = rest[g].astype(jnp.float32)[:, i * tail : (i + 1) * tail]
                matrices[g, i, :, LANES:levels] = piece.astype(jnp.bfloat16)
        near = pl.ds(pl.multiple_of(b * LANES, LANES), LANES)
        far = pl.ds(pl.multiple_of((1 - b) * LANES, LANES), LANES)
        mine = info[g * W + w]

        def two_sources(i, carry):
            k0, k1 = 2 * i, 2 * i + 1
            s0 = lax.rem(w + W - k0, W)
            s1 = lax.rem(w + W - k1, W)
            m0 = info[z * W + s0][pairs : pairs + 1]
            m1 = info[z * W + s1][pairs : pairs + 1]
            m = jnp.concatenate([m0, m1], axis=1)
            x_near = jnp.concatenate(
                [arrived[k0, 0:levels, near], arrived[k1, 0:levels, near]], axis=1
            )
            x_far = jnp.concatenate(
                [arrived[k0, 0:levels, far], arrived[k1, 0:levels, far]], axis=1
            )
            if t == 0:
                y_near = jnp.zeros((solved.shape[1], 2 * LANES), jnp.float32)
                y_far = y_near
            else:
                y_near = jnp.concatenate([solved[k0, :, near], solved[k1, :, near]], axis=1)
                y_far = jnp.concatenate([solved[k0, :, far], solved[k1, :, far]], axis=1)
                y_near = y_near.astype(jnp.float32)
                y_far = y_far.astype(jnp.float32)
            for j in range(pairs):
                low = jnp.concatenate([mine[j : j + 1]] * 2, axis=1)
                here = g * pairs + j - b * block_pairs
                own = wide_pair == here
                use_extra = jnp.logical_and(wide_extra, m == low)
                use_low = jnp.logical_and(jnp.logical_and(own, wide_member == 0), m <= low)
                use_high = jnp.logical_or(own, use_extra)
                lower = jnp.dot(matrices[g, 2 * j], x_near, preferred_element_type=jnp.float32)
                upper = jnp.dot(matrices[g, 2 * j + 1], x_near, preferred_element_type=jnp.float32)
                upper_far = jnp.dot(
                    matrices[g, 2 * j + 1], x_far, preferred_element_type=jnp.float32
                )
                y_near = jnp.where(use_low, lower, jnp.where(use_high, upper, y_near))
                y_far = jnp.where(use_extra, upper_far, y_far)
            y_near = y_near.astype(jnp.bfloat16)
            y_far = y_far.astype(jnp.bfloat16)
            solved[k0, :, near] = y_near[:, :LANES]
            solved[k1, :, near] = y_near[:, LANES:]
            solved[k0, :, far] = y_far[:, :LANES]
            solved[k1, :, far] = y_far[:, LANES:]
            if t == Z - 1:

                @pl.when(i > 0)
                def _():
                    back_copy(k0).start()

                back_copy(k1).start()
            return carry

        lax.fori_loop(0, W // 2, two_sources, 0)

    for t in range(Z):
        if t == Z - 1:
            relay(t)
        solve(t)

    total[...] = jnp.zeros_like(total)

    def collect(k, block):
        if not keep:
            build(k, 0)
        total[...] += lax.dot_general(
            block, pick[place_of(k)], (((1,), (1,)), ((), ())), preferred_element_type=jnp.float32
        )

    collect(0, solved[0])

    def gather_back(k, carry):
        back_copy(k).wait_recv()
        collect(k, returned[k])
        return carry

    lax.fori_loop(1, W, gather_back, 0)

    div = total[0:levels, :].astype(jnp.bfloat16)
    change = jnp.dot(response[...], div, preferred_element_type=jnp.float32)
    old = state[LANES:, :].astype(jnp.float32)
    below = lax.broadcasted_iota(jnp.int32, old.shape, 0) < tail
    new = jnp.where(below, 0.0, old) - change
    new = jnp.where(column_order >= 0, new, 0.0)
    out[0:LANES, :] = div[0:LANES, :]
    out[LANES:, :] = new.astype(jnp.bfloat16)

    def drain(k, carry):
        out_copy(k).wait_send()
        back_copy(k).wait_send()
        return carry

    lax.fori_loop(1, W, drain, 0)

    def drain_info(k, carry):
        info_copy(k).wait_send()
        return carry

    lax.fori_loop(1, devices, drain_info, 0)
    for g in range(Z):
        for c in range(chunks):

            @pl.when(jnp.logical_and(g <= z, z < Z - 1))
            def _():
                z_copy(g, c, 0).wait_send()

            @pl.when(jnp.logical_and(g >= z, z > 0))
            def _():
                z_copy(g, c, 1).wait_send()


def shards(
    state,
    held_orders,
    pair_lows,
    inverses,
    height_operator,
    pressure_column,
    thermal_response_matrix,
    mass_row,
):
    levels = height_operator.shape[0]
    slots = held_orders.shape[0]
    pairs = pair_lows.shape[0]
    Z, W = lax.axis_size("grp"), lax.axis_size("wave")
    devices = Z * W
    width = state.shape[1]
    tail = levels - LANES
    rows = ceil_to(levels, ROWS_TILE)
    height = jnp.concatenate(
        [jnp.zeros((levels, tail), jnp.bfloat16), height_operator, pressure_column[:, None]], axis=1
    )
    through = -jnp.eye(tail, levels, LANES, dtype=jnp.bfloat16)
    response = jnp.concatenate([through, thermal_response_matrix, mass_row[None, :]], axis=0)
    places = W if W * width * 4 * LANES <= KEEP_BYTES else 1
    vmem = pl.BlockSpec(memory_space=pltpu.VMEM)
    smem = pl.BlockSpec(memory_space=pltpu.SMEM)
    block = pltpu.VMEM((W, rows, 2 * LANES), jnp.bfloat16)
    return pl.pallas_call(
        functools.partial(kernel, (Z, W, levels, slots, pairs)),
        out_shape=jax.ShapeDtypeStruct(state.shape, jnp.bfloat16),
        in_specs=[smem, smem, vmem, vmem, vmem, vmem],
        out_specs=vmem,
        scratch_shapes=[
            pltpu.VMEM((devices, pairs + 1, LANES), jnp.int32),
            pltpu.VMEM((Z, 2 * pairs, rows, levels), jnp.bfloat16),
            pltpu.VMEM((Z, rows, LANES), jnp.bfloat16),
            pltpu.VMEM((rows, width), jnp.bfloat16),
            pltpu.VMEM((places, width, 2 * LANES), jnp.bfloat16),
            block,
            block,
            block,
            block,
            pltpu.VMEM((rows, width), jnp.float32),
            pltpu.SemaphoreType.DMA((devices,)),
            pltpu.SemaphoreType.DMA((devices,)),
            pltpu.SemaphoreType.DMA((Z, pairs + 1, 2)),
            pltpu.SemaphoreType.DMA((Z, pairs + 1)),
            pltpu.SemaphoreType.DMA((W,)),
            pltpu.SemaphoreType.DMA((W,)),
            pltpu.SemaphoreType.DMA((W,)),
            pltpu.SemaphoreType.DMA((W,)),
        ],
        compiler_params=pltpu.CompilerParams(
            collective_id=0, has_side_effects=True, vmem_limit_bytes=60 * 1024 * 1024
        ),
    )(
        held_orders,
        pair_lows,
        state,
        inverses.reshape(2 * pairs, levels, levels),
        height,
        response,
    )


def solution(mesh):
    placed = (
        P(None, ("grp", "wave")),
        P(("grp", "wave")),
        P(("grp", "wave")),
        P(("grp", "wave"), None, None, None),
        P(),
        P(),
        P(),
        P(),
    )
    return jax.shard_map(
        shards, mesh=mesh, in_specs=placed, out_specs=P(None, ("grp", "wave")), check_vma=False
    )
```

```python
import functools

import jax
import jax.numpy as jnp
from jax import lax
from jax.experimental import pallas as pl
from jax.experimental.pallas import tpu as pltpu
from jax.sharding import PartitionSpec as P

MESH = pl.DeviceIdType.MESH
LANES = 128
ROWS_TILE = 16
KEEP_BYTES = 24 << 20


def ceil_to(value, step):
    return -(-value // step) * step


def kernel(
    size,
    held,
    lows,
    state_far,
    inverses,
    height_operator,
    pressure_column,
    thermal_response,
    mass_row,
    out,
    state,
    info,
    matrices,
    rest,
    right,
    pick,
    outgoing,
    arrived,
    solved,
    returned,
    total,
    info_send,
    info_recv,
    z_send,
    z_recv,
    out_send,
    out_recv,
    back_send,
    back_recv,
    state_sem,
):
    Z, W, levels, slots, pairs = size
    half_count = Z * W * pairs
    truncation = 2 * half_count - 1
    slot_width = 2 * (truncation + 2)
    width = slots * slot_width
    denom = float(truncation * (truncation + 1))
    devices = Z * W
    per_pair = 4 * slots
    block_pairs = Z * pairs // 2
    first_extra = block_pairs * per_pair
    tail = levels - LANES
    chunks = pairs + 1
    keep = pick.shape[0] > 1
    z = lax.axis_index("grp")
    w = lax.axis_index("wave")
    me = z * W + w

    barrier = pltpu.get_barrier_semaphore()

    def greet(k, carry):
        other = lax.rem(me + k, devices)
        pl.semaphore_signal(
            barrier, inc=1, device_id=(other // W, lax.rem(other, W)), device_id_type=MESH
        )
        return carry

    lax.fori_loop(1, devices, greet, 0)
    fetch = pltpu.make_async_copy(state_far, state, state_sem)
    fetch.start()

    lane = lax.broadcasted_iota(jnp.int32, (1, LANES), 1)
    extra = lane >= first_extra
    used = lane < first_extra + slots
    lane_pair = lane // per_pair
    lane_member = lax.rem(lane, per_pair) // (2 * slots)
    lane_slot = jnp.where(extra, lane - first_extra, lax.rem(lane, 2 * slots) // 2)
    orders = jnp.full((1, LANES), -1, jnp.int32)
    for s in range(slots):
        orders = jnp.where(lane_slot == s, held[s], orders)
    row = lax.broadcasted_iota(jnp.int32, (pairs + 1, LANES), 0)
    tile = jnp.broadcast_to(orders, (pairs + 1, LANES))
    for j in range(pairs):
        tile = jnp.where(row == j, lows[j], tile)
    info[me] = tile

    ends = []
    for i in range(2 * pairs):
        matrices[z, i, 0:levels, :] = inverses[i]
        ends.append(inverses[i, :, LANES:levels].astype(jnp.float32))
    ends = jnp.concatenate(ends, axis=1).astype(jnp.bfloat16)
    rest[z, 0:levels, 0 : 2 * pairs * tail] = ends

    pl.semaphore_wait(barrier, devices - 1)

    def info_copy(k):
        other = lax.rem(me + k, devices)
        return pltpu.make_async_remote_copy(
            src_ref=info.at[me],
            dst_ref=info.at[me],
            send_sem=info_send.at[k],
            recv_sem=info_recv.at[k],
            device_id=(other // W, lax.rem(other, W)),
            device_id_type=MESH,
        )

    def info_arrival(k):
        source = lax.rem(me + devices - k, devices)
        return pltpu.make_async_remote_copy(
            src_ref=info.at[source],
            dst_ref=info.at[source],
            send_sem=info_send.at[k],
            recv_sem=info_recv.at[k],
            device_id=(source // W, lax.rem(source, W)),
            device_id_type=MESH,
        )

    def start_info(k, carry):
        info_copy(k).start()
        return carry

    lax.fori_loop(1, devices, start_info, 0)

    def z_copy(g, c, way):
        if c < pairs:
            ref = matrices.at[g, pl.ds(2 * c, 2), :, pl.ds(0, LANES)]
        else:
            ref = rest.at[g]
        step = 1 if way == 0 else -1
        return pltpu.make_async_remote_copy(
            src_ref=ref,
            dst_ref=ref,
            send_sem=z_send.at[g, c, way],
            recv_sem=z_recv.at[g, c],
            device_id=(z + step, w),
            device_id_type=MESH,
        )

    def forward(g, c):
        @pl.when(jnp.logical_and(g <= z, z < Z - 1))
        def _():
            z_copy(g, c, 0).start()

        @pl.when(jnp.logical_and(g >= z, z > 0))
        def _():
            z_copy(g, c, 1).start()

    def group_at(t):
        g = z
        for zz in range(Z):
            by_distance = sorted(range(Z), key=lambda a: abs(a - zz))
            g = jnp.where(z == zz, by_distance[t], g)
        return g

    def relay(t):
        g = group_at(t)
        for c in range(chunks):
            z_copy(g, c, 0).wait_recv()
            forward(g, c)

    for c in range(chunks):
        forward(z, c)

    column = lax.broadcasted_iota(jnp.int32, (1, width), 1)
    column_order = jnp.full((1, width), -1, jnp.int32)
    column_start = jnp.zeros((1, width), jnp.int32)
    for s in range(slots):
        inside = jnp.logical_and(column >= s * slot_width, column < (s + 1) * slot_width)
        column_order = jnp.where(inside, held[s], column_order)
        column_start = jnp.where(inside, s * slot_width, column_start)
    coefficient = (column - column_start) // 2
    degree = jnp.where(
        coefficient <= truncation - column_order, column_order + coefficient, coefficient - 1
    )
    lap_scale = (degree * (degree + 1)).astype(jnp.float32) / denom
    height = height_operator[...].astype(jnp.float32)
    pressure_row = jnp.broadcast_to(
        pressure_column[...].astype(jnp.float32).reshape(1, levels), height.shape
    )
    across = lax.broadcasted_iota(jnp.int32, height.shape, 1)
    down = lax.broadcasted_iota(jnp.int32, height.shape, 0)
    pressure_side = jnp.sum(
        jnp.where(across == down, pressure_row, 0.0), axis=1, keepdims=True
    )
    height = jnp.concatenate(
        [jnp.zeros((levels, tail), jnp.float32), height, pressure_side], axis=1
    ).astype(jnp.bfloat16)
    fetch.wait()
    drive = jnp.dot(height, state[LANES:, :], preferred_element_type=jnp.float32)
    right[0:levels, :] = (
        state[0:levels, :].astype(jnp.float32) + lap_scale * drive
    ).astype(jnp.bfloat16)

    def wait_info(k, carry):
        info_arrival(k).wait_recv()
        return carry

    lax.fori_loop(1, devices, wait_info, 0)

    def build(k, place):
        d = lax.rem(w + k, W)
        tables = [info[g * W + d] for g in range(Z)]
        low_rows = [tables[g][j : j + 1] for g in range(Z) for j in range(pairs)]
        hit = low_rows[0] == orders
        for low in low_rows[1:]:
            hit = jnp.logical_or(hit, low == orders)
        for b in range(2):
            low = jnp.zeros((1, LANES), jnp.int32)
            for p in range(block_pairs):
                low = jnp.where(lane_pair == p, low_rows[b * block_pairs + p], low)
            merged = jnp.where(orders <= low, low - orders, truncation + 1 - low)
            position = jnp.where(lane_member == 0, merged, truncation - low - orders)
            position = jnp.where(extra, truncation + 1 - orders, position)
            part = jnp.where(extra, b, lax.rem(lane, 2))
            target = lane_slot * slot_width + 2 * position + part
            target = jnp.where(jnp.logical_and(orders >= 0, used), target, -1)
            target = jnp.where(jnp.logical_and(extra, jnp.logical_not(hit)), -1, target)
            at = lax.broadcasted_iota(jnp.int32, (width, LANES), 0)
            pick[place, :, b * LANES : (b + 1) * LANES] = jnp.where(
                at == target, 1.0, 0.0
            ).astype(jnp.bfloat16)

    def place_of(k):
        return k if keep else 0

    def out_copy(k):
        return pltpu.make_async_remote_copy(
            src_ref=outgoing.at[k],
            dst_ref=arrived.at[k],
            send_sem=out_send.at[k],
            recv_sem=out_recv.at[k],
            device_id=(z, lax.rem(w + k, W)),
            device_id_type=MESH,
        )

    def back_copy(k):
        return pltpu.make_async_remote_copy(
            src_ref=solved.at[k],
            dst_ref=returned.at[k],
            send_sem=back_send.at[k],
            recv_sem=back_recv.at[k],
            device_id=(z, lax.rem(w + W - k, W)),
            device_id_type=MESH,
        )

    def message(k):
        build(k, place_of(k))
        return jnp.dot(
            right[...], pick[place_of(k)], preferred_element_type=jnp.float32
        ).astype(jnp.bfloat16)

    def send(k, carry):
        outgoing[k] = message(k)
        out_copy(k).start()
        return carry

    lax.fori_loop(1, W, send, 0)
    arrived[0] = message(0)

    for t in range(1, Z - 1):
        relay(t)

    def wait_out(k, carry):
        out_copy(k).wait_recv()
        return carry

    lax.fori_loop(1, W, wait_out, 0)

    wide_lane = jnp.concatenate([lane, lane], axis=1)
    wide_pair = wide_lane // per_pair
    wide_member = lax.rem(wide_lane, per_pair) // (2 * slots)
    wide_extra = jnp.logical_and(wide_lane >= first_extra, wide_lane < first_extra + slots)

    def solve(t):
        g = group_at(t)
        b = (g * pairs) // block_pairs
        for i in range(2 * pairs):
            if t > 0:
                piece = rest[g].astype(jnp.float32)[:, i * tail : (i + 1) * tail]
                matrices[g, i, :, LANES:levels] = piece.astype(jnp.bfloat16)
        near = pl.ds(pl.multiple_of(b * LANES, LANES), LANES)
        far = pl.ds(pl.multiple_of((1 - b) * LANES, LANES), LANES)
        mine = info[g * W + w]

        def two_sources(i, carry):
            k0, k1 = 2 * i, 2 * i + 1
            s0 = lax.rem(w + W - k0, W)
            s1 = lax.rem(w + W - k1, W)
            m0 = info[z * W + s0][pairs : pairs + 1]
            m1 = info[z * W + s1][pairs : pairs + 1]
            m = jnp.concatenate([m0, m1], axis=1)
            x_near = jnp.concatenate(
                [arrived[k0, 0:levels, near], arrived[k1, 0:levels, near]], axis=1
            )
            x_far = jnp.concatenate(
                [arrived[k0, 0:levels, far], arrived[k1, 0:levels, far]], axis=1
            )
            if t == 0:
                y_near = jnp.zeros((solved.shape[1], 2 * LANES), jnp.float32)
                y_far = y_near
            else:
                y_near = jnp.concatenate([solved[k0, :, near], solved[k1, :, near]], axis=1)
                y_far = jnp.concatenate([solved[k0, :, far], solved[k1, :, far]], axis=1)
                y_near = y_near.astype(jnp.float32)
                y_far = y_far.astype(jnp.float32)
            for j in range(pairs):
                low = jnp.concatenate([mine[j : j + 1]] * 2, axis=1)
                here = g * pairs + j - b * block_pairs
                own = wide_pair == here
                use_extra = jnp.logical_and(wide_extra, m == low)
                use_low = jnp.logical_and(jnp.logical_and(own, wide_member == 0), m <= low)
                use_high = jnp.logical_or(own, use_extra)
                lower = jnp.dot(matrices[g, 2 * j], x_near, preferred_element_type=jnp.float32)
                upper = jnp.dot(matrices[g, 2 * j + 1], x_near, preferred_element_type=jnp.float32)
                upper_far = jnp.dot(
                    matrices[g, 2 * j + 1], x_far, preferred_element_type=jnp.float32
                )
                y_near = jnp.where(use_low, lower, jnp.where(use_high, upper, y_near))
                y_far = jnp.where(use_extra, upper_far, y_far)
            y_near = y_near.astype(jnp.bfloat16)
            y_far = y_far.astype(jnp.bfloat16)
            solved[k0, :, near] = y_near[:, :LANES]
            solved[k1, :, near] = y_near[:, LANES:]
            solved[k0, :, far] = y_far[:, :LANES]
            solved[k1, :, far] = y_far[:, LANES:]
            if t == Z - 1:

                @pl.when(i > 0)
                def _():
                    back_copy(k0).start()

                back_copy(k1).start()
            return carry

        lax.fori_loop(0, W // 2, two_sources, 0)

    for t in range(Z):
        if t == Z - 1:
            relay(t)
        solve(t)

    total[...] = jnp.zeros_like(total)
    through_row = lax.broadcasted_iota(jnp.int32, (tail, levels), 0)
    through_lane = lax.broadcasted_iota(jnp.int32, (tail, levels), 1)
    response = jnp.concatenate(
        [
            jnp.where(through_lane == through_row + LANES, -1.0, 0.0),
            thermal_response[...].astype(jnp.float32),
            mass_row[...].astype(jnp.float32).reshape(1, levels),
        ],
        axis=0,
    ).astype(jnp.bfloat16)

    def collect(k, block):
        if not keep:
            build(k, 0)
        total[...] += lax.dot_general(
            block, pick[place_of(k)], (((1,), (1,)), ((), ())), preferred_element_type=jnp.float32
        )

    collect(0, solved[0])

    def gather_back(k, carry):
        back_copy(k).wait_recv()
        collect(k, returned[k])
        return carry

    lax.fori_loop(1, W, gather_back, 0)

    div = total[0:levels, :].astype(jnp.bfloat16)
    change = jnp.dot(response, div, preferred_element_type=jnp.float32)
    old = state[LANES:, :].astype(jnp.float32)
    below = lax.broadcasted_iota(jnp.int32, old.shape, 0) < tail
    new = jnp.where(below, 0.0, old) - change
    new = jnp.where(column_order >= 0, new, 0.0)
    out[0:LANES, :] = div[0:LANES, :]
    out[LANES:, :] = new.astype(jnp.bfloat16)

    def drain(k, carry):
        out_copy(k).wait_send()
        back_copy(k).wait_send()
        return carry

    lax.fori_loop(1, W, drain, 0)

    def drain_info(k, carry):
        info_copy(k).wait_send()
        return carry

    lax.fori_loop(1, devices, drain_info, 0)
    for g in range(Z):
        for c in range(chunks):

            @pl.when(jnp.logical_and(g <= z, z < Z - 1))
            def _():
                z_copy(g, c, 0).wait_send()

            @pl.when(jnp.logical_and(g >= z, z > 0))
            def _():
                z_copy(g, c, 1).wait_send()


def shards(
    state,
    held_orders,
    pair_lows,
    inverses,
    height_operator,
    pressure_column,
    thermal_response_matrix,
    mass_row,
):
    levels = height_operator.shape[0]
    slots = held_orders.shape[0]
    pairs = pair_lows.shape[0]
    Z, W = lax.axis_size("grp"), lax.axis_size("wave")
    devices = Z * W
    width = state.shape[1]
    rows = ceil_to(levels, ROWS_TILE)
    places = W if W * width * 4 * LANES <= KEEP_BYTES else 1
    vmem = pl.BlockSpec(memory_space=pltpu.VMEM)
    smem = pl.BlockSpec(memory_space=pltpu.SMEM)
    block = pltpu.VMEM((W, rows, 2 * LANES), jnp.bfloat16)
    return pl.pallas_call(
        functools.partial(kernel, (Z, W, levels, slots, pairs)),
        out_shape=jax.ShapeDtypeStruct(state.shape, jnp.bfloat16),
        in_specs=[smem, smem, pl.BlockSpec(memory_space=pl.ANY)] + [vmem] * 5,
        out_specs=vmem,
        scratch_shapes=[
            pltpu.VMEM(state.shape, jnp.bfloat16),
            pltpu.VMEM((devices, pairs + 1, LANES), jnp.int32),
            pltpu.VMEM((Z, 2 * pairs, rows, levels), jnp.bfloat16),
            pltpu.VMEM((Z, rows, LANES), jnp.bfloat16),
            pltpu.VMEM((rows, width), jnp.bfloat16),
            pltpu.VMEM((places, width, 2 * LANES), jnp.bfloat16),
            block,
            block,
            block,
            block,
            pltpu.VMEM((rows, width), jnp.float32),
            pltpu.SemaphoreType.DMA((devices,)),
            pltpu.SemaphoreType.DMA((devices,)),
            pltpu.SemaphoreType.DMA((Z, pairs + 1, 2)),
            pltpu.SemaphoreType.DMA((Z, pairs + 1)),
            pltpu.SemaphoreType.DMA((W,)),
            pltpu.SemaphoreType.DMA((W,)),
            pltpu.SemaphoreType.DMA((W,)),
            pltpu.SemaphoreType.DMA((W,)),
            pltpu.SemaphoreType.DMA,
        ],
        compiler_params=pltpu.CompilerParams(
            collective_id=0, has_side_effects=True, vmem_limit_bytes=60 * 1024 * 1024
        ),
    )(
        held_orders,
        pair_lows,
        state,
        inverses.reshape(2 * pairs, levels, levels),
        height_operator,
        pressure_column,
        thermal_response_matrix,
        mass_row,
    )


def solution(mesh):
    placed = (
        P(None, ("grp", "wave")),
        P(("grp", "wave")),
        P(("grp", "wave")),
        P(("grp", "wave"), None, None, None),
        P(),
        P(),
        P(),
        P(),
    )
    return jax.shard_map(
        shards, mesh=mesh, in_specs=placed, out_specs=P(None, ("grp", "wave")), check_vma=False
    )
```
